128 devices in a mesh: row: 8 (over x, y_lo), col: 16 (over y_hi, z, core).
Axes of the slice: x: 4, y: 4 (y_hi: 2, y_lo: 2; y = y_hi * 2 + y_lo), z: 4, core: 2. Of those that a mesh axis runs over, the one named last changes fastest.
Arguments:
- train_table: bfloat16 [8, 256, 262144], P('row', 'col'), may hold values from -6 to 6
- token_ids: int32 [512], replicated, may hold values from 0 to 262143
- hidden: bfloat16 [8, 512, 2560], P('row', 'col'), may hold values from -6 to 6
- w_gate: bfloat16 [8, 2560, 256], P('row'), may hold values from -0.125 to 0.125
- w_proj: bfloat16 [8, 256, 2560], P('row'), may hold values from -0.375 to 0.375
- gain: bfloat16 [8, 2560], P('row'), may hold values from 0.5 to 1.5
Outputs:
- serve_table: bfloat16 [8, 256, 262144], P(None, None, ('row', 'col'))
- update: bfloat16 [8, 512, 2560], P('row', 'col')
The draws below stay inside these ranges and needn't reach their ends.
All inputs are finite; a program needn't handle non-finite values.
Results may differ from the reference program's by a relative error of at most 0.0048.
Values may be sent and summed in bfloat16 or wider, within the bound.
No kernel may reach another device: no remote copies, remote signals or barrier semaphores. Data moves between devices by JAX's collectives and lax.ppermute only.
A program may use at most 256 MiB of HBM per device.

```python
import jax
import jax.numpy as jnp
from jax import lax

VOCAB = 262144
P_SIZE = 256
D = 2560
L = 8
TOKENS = 512


def touch_ends(array, stream_key, least, largest):
    longest = array.shape.index(max(array.shape))
    spots = []
    for shift in (0, 1):
        where = [jax.random.randint(jax.random.fold_in(stream_key, axis), (), 0, length) for axis, length in enumerate(array.shape)]
        where[longest] = (where[longest] + shift) % array.shape[longest]
        spots.append(tuple(where))
    return array.at[spots[0]].set(least).at[spots[1]].set(largest)


def levels(own_key, extent, shards, smallest, high):
    level = 1.0
    for axis_at, blocks in shards:
        heights = jax.random.uniform(jax.random.fold_in(jax.random.fold_in(own_key, 6), axis_at), (blocks,), jnp.float32, smallest / len(shards), high / len(shards))
        level = level * jnp.repeat(jnp.exp(heights), extent[axis_at] // blocks).reshape((-1,) + (1,) * (len(extent) - 1 - axis_at))
    return level


def gaussian(own_key, dims, scale, most, cuts=(), kind=jnp.bfloat16):
    entries = jax.random.normal(own_key, dims, jnp.float32) * scale
    if len(cuts) > 0:
        entries = levels(own_key, dims, cuts, -0.22, 0.18) * entries
    return jnp.clip(entries, min=-most, max=most).astype(kind)


def setup_inputs(seed: int = 0) -> dict:
    arg_keys = jax.random.split(jax.random.key(seed), 7)
    return {
        "train_table": gaussian(arg_keys[0], (L, P_SIZE, VOCAB), 1.0, 6.0, ((0, 8), (1, 16))),
        "token_ids": touch_ends(jax.random.randint(arg_keys[1], (TOKENS,), 0, VOCAB), jax.random.fold_in(arg_keys[1], 1), 0, VOCAB - 1).astype(jnp.int32),
        "hidden": gaussian(arg_keys[2], (L, TOKENS, D), 1.0, 6.0, ((0, 8), (1, 16))),
        "w_gate": gaussian(arg_keys[3], (L, D, P_SIZE), D ** -0.5, 0.125, ((0, 8),)),
        "w_proj": gaussian(arg_keys[4], (L, P_SIZE, D), P_SIZE ** -0.5, 0.375, ((0, 8),)),
        "gain": jnp.clip(1.0 + 0.1 * jax.random.normal(arg_keys[5], (L, D), jnp.float32), 0.5, 1.5).astype(jnp.bfloat16),
    }


def reference(train_table, token_ids, hidden, w_gate, w_proj, gain):
    emb = jnp.take(train_table, token_ids.astype(jnp.int32), axis=2).astype(jnp.float32)
    emb = jnp.transpose(emb, (0, 2, 1))
    gate_pre = jnp.einsum('ltd,ldp->ltp', hidden.astype(jnp.float32), w_gate.astype(jnp.float32))
    gated = jax.nn.gelu(gate_pre, approximate=True)
    mixed = (gated * emb).astype(jnp.bfloat16)
    projected = jnp.einsum('ltp,lpd->ltd', mixed.astype(jnp.float32), w_proj.astype(jnp.float32))
    inverse_rms = jax.lax.rsqrt(lax.optimization_barrier(jnp.mean(projected * projected, axis=-1, keepdims=True)) + 1e-06)
    update = (projected * inverse_rms * gain.astype(jnp.float32)[:, None, :]).astype(jnp.bfloat16)
    return (train_table, update)
```

```python
import jax
import jax.numpy as jnp
from jax import lax
from jax.experimental import pallas as pl
from jax.experimental.pallas import tpu as pltpu
from jax.sharding import PartitionSpec as P

LANES = 128


def pick_kernel(ids_ref, table_ref, out_ref, tiles, sem):
    tokens = ids_ref.shape[0]
    columns = table_ref.shape[1]

    @pl.loop(0, tokens, unroll=8)
    def _(t):
        start = pl.multiple_of((ids_ref[t] // LANES) * LANES, LANES)
        pltpu.make_async_copy(table_ref.at[0, :, pl.ds(start, LANES)], tiles.at[t], sem).start()

    pltpu.make_async_copy(tiles, tiles, sem).wait()
    lane = lax.broadcasted_iota(jnp.int32, (columns, LANES), 1)
    for block in range(tokens // LANES):

        def step(i, acc):
            t = block * LANES + i
            at = ids_ref[t] % LANES
            turned = pltpu.roll(tiles[t].astype(jnp.float32), (i - at + LANES) % LANES, 1)
            return jnp.where(lane == i, turned, acc)

        acc = lax.fori_loop(0, LANES, step, jnp.zeros((columns, LANES), jnp.float32), unroll=8)
        out_ref[:, block * LANES:(block + 1) * LANES] = acc.astype(jnp.bfloat16)


def pick_columns(token_ids, train_table):
    tokens = token_ids.shape[0]
    columns = train_table.shape[1]
    return pl.pallas_call(
        pick_kernel,
        out_shape=jax.ShapeDtypeStruct((columns, tokens), jnp.bfloat16),
        in_specs=[pl.BlockSpec(memory_space=pltpu.SMEM), pl.BlockSpec(memory_space=pl.ANY)],
        out_specs=pl.BlockSpec(memory_space=pltpu.VMEM),
        scratch_shapes=[pltpu.VMEM((tokens, columns, LANES), jnp.bfloat16), pltpu.SemaphoreType.DMA],
        cost_estimate=pl.CostEstimate(flops=20_000_000, bytes_accessed=2 << 20, transcendentals=0),
    )(token_ids, train_table)


def shards(train_table, token_ids, hidden, w_gate, w_proj, gain):
    row_count = lax.axis_size("row")
    col_count = lax.axis_size("col")
    devices_all = row_count * col_count
    columns = train_table.shape[1]
    local_vocab = train_table.shape[2] // devices_all
    shaped = train_table.reshape(columns // 8, 8, devices_all, local_vocab)
    shaped = jnp.transpose(shaped, (2, 0, 1, 3))
    arrived = lax.all_to_all(shaped, ("row", "col"), split_axis=0, concat_axis=0, tiled=True)
    served = arrived.reshape(row_count, col_count * columns, local_vocab)
    picked = pick_columns(token_ids, train_table)
    picked = picked.reshape(columns, col_count, picked.shape[1] // col_count)
    owned = lax.all_to_all(picked, "col", split_axis=1, concat_axis=0, tiled=True)
    owned = owned.reshape(owned.shape[0], owned.shape[2])
    emb = jnp.transpose(owned).astype(jnp.float32)
    current = hidden[0]
    gate_pre = jnp.dot(current, w_gate[0], preferred_element_type=jnp.float32)
    gated = jax.nn.gelu(gate_pre, approximate=True)
    mixed = (gated * emb).astype(jnp.bfloat16)
    projected = jnp.dot(mixed, w_proj[0], preferred_element_type=jnp.float32)
    inverse_rms = lax.rsqrt(jnp.mean(projected * projected, axis=-1, keepdims=True) + 1e-06)
    update = (projected * inverse_rms * gain[0].astype(jnp.float32)[None, :]).astype(jnp.bfloat16)
    return (served, update[None])


def solution(mesh):
    in_specs = (
        P("row", "col", None),
        P(),
        P("row", "col", None),
        P("row", None, None),
        P("row", None, None),
        P("row", None),
    )
    out_specs = (P(None, None, ("row", "col")), P("row", "col", None))
    return jax.shard_map(shards, mesh=mesh, in_specs=in_specs, out_specs=out_specs, check_vma=False)
```

```python
import jax
import jax.numpy as jnp
from jax import lax
from jax.experimental import pallas as pl
from jax.experimental.pallas import tpu as pltpu
from jax.sharding import PartitionSpec as P

LANES = 128
SUBLANES = 8
MIB = 1 << 20
ROWS, COLS = 8, 16


def spot(row, col):
    return row * COLS + col


def owner(i):
    return i


def head_kernel(ids_ref, table_ref, out_ref, sem):
    parts, tiles = out_ref.shape[:2]
    tokens = ids_ref.shape[0]
    halves = table_ref.shape[0]
    local = (tiles - 1) // halves

    @pl.loop(0, parts, unroll=4)
    def _(i):
        start = owner(i) * local
        for h in range(halves):
            pltpu.make_async_copy(
                table_ref.at[h, pl.ds(start, local)], out_ref.at[i, pl.ds(h * local, local)], sem
            ).start()

    whole = out_ref.at[:, pl.ds(0, halves * local)]
    pltpu.make_async_copy(whole, whole, sem).wait()

    me = lax.axis_index("row")
    lane = lax.broadcasted_iota(jnp.int32, (SUBLANES, LANES), 1)
    here = tokens // COLS
    for block in range(tokens // LANES):

        def step(i, accs):
            at = ids_ref[block * LANES + i]
            tile = lax.shift_right_logical(at, 7)
            part = spot(lax.shift_right_logical(tile, 8), lax.bitwise_and(lax.shift_right_logical(tile, 4), COLS - 1))
            inner = lax.bitwise_and(tile, local - 1)
            turn = lax.bitwise_and(i - at, LANES - 1)
            hit = lane == i
            out = []
            for h, acc in enumerate(accs):
                turned = pltpu.roll(out_ref[part, inner + h * local].astype(jnp.float32), turn, 1)
                out.append(jnp.where(hit, turned, acc))
            return tuple(out)

        zero = jnp.zeros((SUBLANES, LANES), jnp.float32)
        low, high = lax.fori_loop(0, LANES, step, (zero, zero), unroll=8)
        high = pltpu.roll(high, here, 1)
        for s in range(LANES // here):
            mine = (lane >= s * here) & (lane < (s + 1) * here)
            packed = jnp.where(mine, low, high).astype(jnp.bfloat16)
            out_ref[spot(me, block * (LANES // here) + s), tiles - 1] = packed


def head(token_ids, table):
    halves, tiles = table.shape[:2]
    parts = ROWS * COLS
    return pl.pallas_call(
        head_kernel,
        out_shape=pltpu.VMEM((parts, halves * tiles // parts + 1, SUBLANES, LANES), jnp.bfloat16),
        in_specs=[pl.BlockSpec(memory_space=pltpu.SMEM), pl.BlockSpec(memory_space=pl.ANY)],
        out_specs=pl.BlockSpec(memory_space=pltpu.VMEM),
        scratch_shapes=[pltpu.SemaphoreType.DMA],
        cost_estimate=pl.CostEstimate(flops=20 * MIB, bytes_accessed=16 * MIB, transcendentals=0),
        compiler_params=pltpu.CompilerParams(vmem_limit_bytes=16 * MIB),
    )(token_ids, pltpu.with_memory_space_constraint(table, pltpu.HBM))


def tail_kernel(arrived_ref, hidden_ref, gate_ref, proj_ref, gain_ref, served_ref, update_ref, emb_ref, sem):
    parts, tiles = arrived_ref.shape[:2]

    @pl.loop(0, ROWS)
    def _(row):
        @pl.loop(0, COLS, unroll=8)
        def _(col):
            pltpu.make_async_copy(
                arrived_ref.at[spot(row, col), pl.ds(0, tiles - 1)], served_ref.at[row, col], sem
            ).start()

    gate_pre = jnp.dot(hidden_ref[0], gate_ref[0], preferred_element_type=jnp.float32)
    gated = jax.nn.gelu(gate_pre, approximate=True)
    here = gated.shape[0]
    me, share = lax.axis_index("col"), LANES // here
    row = lax.axis_index("row")
    turn = lax.rem(share - lax.rem(me, share), share) * here
    for col in range(COLS):
        tile = arrived_ref[spot(row, col), tiles - 1].astype(jnp.float32)
        low = pltpu.roll(tile, turn, 1)
        emb_ref[2 * col * SUBLANES:(2 * col + 1) * SUBLANES] = low
        emb_ref[(2 * col + 1) * SUBLANES:(2 * col + 2) * SUBLANES] = pltpu.roll(low, LANES - here, 1)
    emb = jnp.transpose(emb_ref[...])[:here]
    mixed = (gated * emb).astype(jnp.bfloat16)
    projected = jnp.dot(mixed, proj_ref[0], preferred_element_type=jnp.float32)
    inverse_rms = lax.rsqrt(jnp.mean(projected * projected, axis=-1, keepdims=True) + 1e-06)
    update_ref[0] = (projected * inverse_rms * gain_ref[...].astype(jnp.float32)).astype(jnp.bfloat16)
    pltpu.make_async_copy(served_ref, served_ref, sem).wait()


def tail(arrived, hidden, w_gate, w_proj, gain):
    tiles = arrived.shape[1] - 1
    return pl.pallas_call(
        tail_kernel,
        out_shape=[
            pltpu.HBM((ROWS, COLS, tiles, SUBLANES, LANES), jnp.bfloat16),
            jax.ShapeDtypeStruct(hidden.shape, jnp.bfloat16),
        ],
        in_specs=[pl.BlockSpec(memory_space=pltpu.VMEM)] * 5,
        out_specs=[pl.BlockSpec(memory_space=pl.ANY), pl.BlockSpec(memory_space=pltpu.VMEM)],
        scratch_shapes=[pltpu.VMEM((w_gate.shape[2], LANES), jnp.float32), pltpu.SemaphoreType.DMA],
        cost_estimate=pl.CostEstimate(flops=100 * MIB, bytes_accessed=18 * MIB, transcendentals=0),
        compiler_params=pltpu.CompilerParams(vmem_limit_bytes=24 * MIB),
    )(pltpu.with_memory_space_constraint(arrived, pltpu.VMEM), hidden, w_gate, w_proj, gain)


def shards(train_table, token_ids, hidden, w_gate, w_proj, gain):
    columns, vocab = train_table.shape[1:]
    parts = ROWS * COLS
    halves, tiles = columns // SUBLANES, vocab // LANES
    table = jnp.transpose(train_table.reshape(halves, SUBLANES, tiles, LANES), (0, 2, 1, 3))
    blocks = head(token_ids, table)
    arrived = lax.all_to_all(blocks, ("row", "col"), split_axis=0, concat_axis=0, tiled=True)
    served, update = tail(arrived, hidden, w_gate, w_proj, gain)
    served = served.reshape(ROWS, COLS, halves, tiles // parts, SUBLANES, LANES)
    served = jnp.transpose(served, (0, 1, 2, 4, 3, 5)).reshape(ROWS, COLS * columns, vocab // parts)
    return (served, update)


def solution(mesh):
    in_specs = (
        P("row", "col", None),
        P(),
        P("row", "col", None),
        P("row", None, None),
        P("row", None, None),
        P("row", None),
    )
    out_specs = (P(None, None, ("row", "col")), P("row", "col", None))
    return jax.shard_map(shards, mesh=mesh, in_specs=in_specs, out_specs=out_specs, check_vma=False)
```

```python
import jax
import jax.numpy as jnp
from jax import lax
from jax.experimental import pallas as pl
from jax.experimental.pallas import tpu as pltpu
from jax.sharding import PartitionSpec as P

LANES = 128
SUBLANES = 8
MIB = 1 << 20
ROWS, COLS = 8, 16


def in_hbm(array):
    return pltpu.with_memory_space_constraint(array, pltpu.HBM)


def head_kernel(ids_ref, table_ref, out_ref, ids, tile_of, turn_of, sem, ids_sem):
    halves, parts, local = table_ref.shape[:3]
    tokens = ids.shape[0]
    pieces = 8
    size = parts // pieces
    for p in range(pieces):
        for h in range(halves):
            pltpu.make_async_copy(
                table_ref.at[h, pl.ds(p * size, size)],
                out_ref.at[pl.ds(p * size, size), pl.ds(h * local, local)],
                sem,
            ).start()
    fetch = pltpu.make_async_copy(ids_ref, ids, ids_sem)
    fetch.start()
    fetch.wait()

    @pl.loop(0, tokens, unroll=8)
    def _(t):
        at = ids[t]
        tile = lax.shift_right_logical(at, 7)
        tile_of[t] = tile + (halves * local + 1 - local) * lax.shift_right_logical(tile, 4)
        turn_of[t] = lax.bitwise_and(t - at, LANES - 1)

    flat = out_ref.reshape(parts * (halves * local + 1), SUBLANES, LANES)
    whole = out_ref.at[:, pl.ds(0, halves * local)]
    pltpu.make_async_copy(whole, whole, sem).wait()

    row = lax.axis_index("row")
    lane = lax.broadcasted_iota(jnp.int32, (SUBLANES, LANES), 1)
    here = tokens // COLS
    peers = LANES // here

    @pl.loop(0, tokens // LANES)
    def _(block):
        accs = [jnp.zeros((SUBLANES, LANES), jnp.float32)] * halves
        for i in range(LANES):
            tile, turn = tile_of[block * LANES + i], turn_of[block * LANES + i]
            for h in range(halves):
                turned = pltpu.roll(flat[tile + h * local].astype(jnp.float32), turn, 1)
                accs[h] = jnp.where(lane == i, turned, accs[h])
        low, high = accs[0], pltpu.roll(accs[1], here, 1)
        for s in range(peers):
            mine = (lane >= s * here) & (lane < (s + 1) * here)
            packed = jnp.where(mine, low, high).astype(jnp.bfloat16)
            out_ref[row * COLS + block * peers + s, halves * local] = packed


def head(token_ids, table):
    halves, parts, local = table.shape[:3]
    tokens = token_ids.shape[0]
    return pl.pallas_call(
        head_kernel,
        out_shape=pltpu.VMEM((parts, halves * local + 1, SUBLANES, LANES), jnp.bfloat16),
        in_specs=[pl.BlockSpec(memory_space=pl.ANY)] * 2,
        out_specs=pl.BlockSpec(memory_space=pltpu.VMEM),
        scratch_shapes=[pltpu.SMEM((tokens,), jnp.int32)] * 3 + [pltpu.SemaphoreType.DMA] * 2,
        cost_estimate=pl.CostEstimate(flops=20 * MIB, bytes_accessed=16 * MIB, transcendentals=0),
        compiler_params=pltpu.CompilerParams(vmem_limit_bytes=16 * MIB),
    )(in_hbm(token_ids), in_hbm(table))


def tail_kernel(arrived_ref, hidden_ref, gate_ref, proj_ref, gain_ref, served_ref, update_ref, emb_ref, sem):
    parts, tiles = arrived_ref.shape[:2]

    @pl.loop(0, ROWS)
    def _(row):
        @pl.loop(0, COLS, unroll=8)
        def _(col):
            pltpu.make_async_copy(
                arrived_ref.at[row * COLS + col, pl.ds(0, tiles - 1)], served_ref.at[row, col], sem
            ).start()

    gate_pre = jnp.dot(hidden_ref[0], gate_ref[0], preferred_element_type=jnp.float32)
    gated = jax.nn.gelu(gate_pre, approximate=True)
    here = gated.shape[0]
    me, share = lax.axis_index("col"), LANES // here
    row = lax.axis_index("row")
    turn = lax.rem(share - lax.rem(me, share), share) * here
    for col in range(COLS):
        tile = arrived_ref[row * COLS + col, tiles - 1].astype(jnp.float32)
        low = pltpu.roll(tile, turn, 1)
        emb_ref[2 * col * SUBLANES:(2 * col + 1) * SUBLANES] = low
        emb_ref[(2 * col + 1) * SUBLANES:(2 * col + 2) * SUBLANES] = pltpu.roll(low, LANES - here, 1)
    emb = jnp.transpose(emb_ref[...])[:here]
    mixed = (gated * emb).astype(jnp.bfloat16)
    projected = jnp.dot(mixed, proj_ref[0], preferred_element_type=jnp.float32)
    inverse_rms = lax.rsqrt(jnp.mean(projected * projected, axis=-1, keepdims=True) + 1e-06)
    update_ref[0] = (projected * inverse_rms * gain_ref[...].astype(jnp.float32)).astype(jnp.bfloat16)
    pltpu.make_async_copy(served_ref, served_ref, sem).wait()


def tail(arrived, hidden, w_gate, w_proj, gain):
    tiles = arrived.shape[1] - 1
    return pl.pallas_call(
        tail_kernel,
        out_shape=[
            pltpu.HBM((ROWS, COLS, tiles, SUBLANES, LANES), jnp.bfloat16),
            jax.ShapeDtypeStruct(hidden.shape, jnp.bfloat16),
        ],
        in_specs=[pl.BlockSpec(memory_space=pltpu.VMEM)] * 5,
        out_specs=[pl.BlockSpec(memory_space=pl.ANY), pl.BlockSpec(memory_space=pltpu.VMEM)],
        scratch_shapes=[pltpu.VMEM((w_gate.shape[2], LANES), jnp.float32), pltpu.SemaphoreType.DMA],
        cost_estimate=pl.CostEstimate(flops=100 * MIB, bytes_accessed=18 * MIB, transcendentals=0),
        compiler_params=pltpu.CompilerParams(vmem_limit_bytes=24 * MIB),
    )(pltpu.with_memory_space_constraint(arrived, pltpu.VMEM), hidden, w_gate, w_proj, gain)


def shards(train_table, token_ids, hidden, w_gate, w_proj, gain):
    columns, vocab = train_table.shape[1:]
    parts = ROWS * COLS
    halves, tiles = columns // SUBLANES, vocab // LANES
    table = jnp.transpose(train_table.reshape(halves, SUBLANES, tiles, LANES), (0, 2, 1, 3))
    table = table.reshape(halves, parts, tiles // parts, SUBLANES, LANES)
    blocks = head(token_ids, table)
    arrived = lax.all_to_all(blocks, ("row", "col"), split_axis=0, concat_axis=0, tiled=True)
    served, update = tail(arrived, hidden, w_gate, w_proj, gain)
    served = served.reshape(ROWS, COLS, halves, tiles // parts, SUBLANES, LANES)
    served = jnp.transpose(served, (0, 1, 2, 4, 3, 5)).reshape(ROWS, COLS * columns, vocab // parts)
    return (served, update)


def solution(mesh):
    in_specs = (
        P("row", "col", None),
        P(),
        P("row", "col", None),
        P("row", None, None),
        P("row", None, None),
        P("row", None),
    )
    out_specs = (P(None, None, ("row", "col")), P("row", "col", None))
    return jax.shard_map(shards, mesh=mesh, in_specs=in_specs, out_specs=out_specs, check_vma=False)
```

```python
import jax
import jax.numpy as jnp
from jax import lax
from jax.experimental import pallas as pl
from jax.experimental.pallas import tpu as pltpu
from jax.sharding import PartitionSpec as P

LANES = 128
SUBLANES = 4
MIB = 1 << 20
ROWS, COLS = 8, 16


def in_hbm(array):
    return pltpu.with_memory_space_constraint(array, pltpu.HBM)


def head_kernel(ids_ref, table_ref, out_ref, ids, tile_of, turn_of, sem, ids_sem):
    halves, parts, local = table_ref.shape[:3]
    tokens = ids.shape[0]
    pieces = 8
    size = parts // pieces
    for p in range(pieces):
        for h in range(halves):
            pltpu.make_async_copy(
                table_ref.at[h, pl.ds(p * size, size)],
                out_ref.at[pl.ds(p * size, size), pl.ds(h * local, local)],
                sem,
            ).start()
    fetch = pltpu.make_async_copy(ids_ref, ids, ids_sem)
    fetch.start()
    fetch.wait()

    @pl.loop(0, tokens, unroll=8)
    def _(t):
        at = ids[t]
        tile = lax.shift_right_logical(at, 7)
        tile_of[t] = 2 * tile + (halves * local + 1 - local) * lax.shift_right_logical(tile, 4)
        turn_of[t] = lax.bitwise_and(t - at, LANES - 1)

    flat = out_ref.reshape(parts * (halves * local + 1), SUBLANES, LANES)
    whole = out_ref.at[:, pl.ds(0, halves * local)]
    pltpu.make_async_copy(whole, whole, sem).wait()

    row = lax.axis_index("row")
    lane = lax.broadcasted_iota(jnp.int32, (SUBLANES, LANES), 1)
    here = tokens // COLS
    peers = LANES // here

    @pl.loop(0, tokens // LANES)
    def _(block):
        accs = [jnp.zeros((SUBLANES, LANES), jnp.float32)] * (2 * halves)
        for i in range(LANES):
            tile, turn = tile_of[block * LANES + i], turn_of[block * LANES + i]
            for k in range(2 * halves):
                turned = pltpu.roll(flat[tile + k // 2 * local + k % 2].astype(jnp.float32), turn, 1)
                accs[k] = jnp.where(lane == i, turned, accs[k])
        accs = [pltpu.roll(acc, k * here, 1) if k else acc for k, acc in enumerate(accs)]
        for s in range(peers):
            packed = accs[-1]
            for k in range(2 * halves - 1):
                packed = jnp.where(lane // here == (s + k) % peers, accs[k], packed)
            out_ref[row * COLS + block * peers + s, halves * local] = packed.astype(jnp.bfloat16)


def head(token_ids, table):
    halves, parts, local = table.shape[:3]
    tokens = token_ids.shape[0]
    return pl.pallas_call(
        head_kernel,
        out_shape=pltpu.VMEM((parts, halves * local + 1, SUBLANES, LANES), jnp.bfloat16),
        in_specs=[pl.BlockSpec(memory_space=pl.ANY)] * 2,
        out_specs=pl.BlockSpec(memory_space=pltpu.VMEM),
        scratch_shapes=[pltpu.SMEM((tokens,), jnp.int32)] * 3 + [pltpu.SemaphoreType.DMA] * 2,
        cost_estimate=pl.CostEstimate(flops=20 * MIB, bytes_accessed=16 * MIB, transcendentals=0),
        compiler_params=pltpu.CompilerParams(vmem_limit_bytes=16 * MIB),
    )(in_hbm(token_ids), in_hbm(table))


def tail_kernel(arrived_ref, hidden_ref, gate_ref, proj_ref, gain_ref, served_ref, update_ref, emb_ref, branch_ref, sems, update_sem):
    tiles = arrived_ref.shape[1]
    halfway = ROWS // 2

    @pl.loop(0, ROWS)
    def _(row):
        @pl.loop(0, COLS, unroll=8)
        def _(col):
            pltpu.make_async_copy(
                arrived_ref.at[row * COLS + col, pl.ds(0, tiles - 1)], served_ref.at[row, col], sems.at[row // halfway]
            ).start()

    gate_pre = jnp.dot(hidden_ref[0], gate_ref[0], preferred_element_type=jnp.float32)
    gated = jax.nn.gelu(gate_pre, approximate=True)
    here = gated.shape[0]
    me, share = lax.axis_index("col"), LANES // here
    row = lax.axis_index("row")
    turn = lax.rem(share - lax.rem(me, share), share) * here
    for col in range(COLS):
        tile = arrived_ref[row * COLS + col, tiles - 1].astype(jnp.float32)
        low = pltpu.roll(tile, turn, 1)
        for k in range(share):
            start = (col * share + k) * SUBLANES
            emb_ref[start:start + SUBLANES] = pltpu.roll(low, (LANES - k * here) % LANES, 1) if k else low
    emb = jnp.transpose(emb_ref[...])[:here]
    mixed = (gated * emb).astype(jnp.bfloat16)
    projected = jnp.dot(mixed, proj_ref[0], preferred_element_type=jnp.float32)
    inverse_rms = lax.rsqrt(jnp.mean(projected * projected, axis=-1, keepdims=True) + 1e-06)
    branch_ref[0] = (projected * inverse_rms * gain_ref[...].astype(jnp.float32)).astype(jnp.bfloat16)
    first, second = served_ref.at[pl.ds(0, halfway)], served_ref.at[pl.ds(halfway, halfway)]
    pltpu.make_async_copy(first, first, sems.at[0]).wait()
    send = pltpu.make_async_copy(branch_ref, update_ref, update_sem)
    send.start()
    pltpu.make_async_copy(second, second, sems.at[1]).wait()
    send.wait()


def tail(arrived, hidden, w_gate, w_proj, gain):
    tiles = arrived.shape[1] - 1
    return pl.pallas_call(
        tail_kernel,
        out_shape=[
            pltpu.HBM((ROWS, COLS, tiles, SUBLANES, LANES), jnp.bfloat16),
            pltpu.HBM(hidden.shape, jnp.bfloat16),
        ],
        in_specs=[pl.BlockSpec(memory_space=pltpu.VMEM)] * 5,
        out_specs=[pl.BlockSpec(memory_space=pl.ANY)] * 2,
        scratch_shapes=[
            pltpu.VMEM((w_gate.shape[2], LANES), jnp.float32),
            pltpu.VMEM(hidden.shape, jnp.bfloat16),
            pltpu.SemaphoreType.DMA((2,)),
            pltpu.SemaphoreType.DMA,
        ],
        cost_estimate=pl.CostEstimate(flops=100 * MIB, bytes_accessed=18 * MIB, transcendentals=0),
        compiler_params=pltpu.CompilerParams(vmem_limit_bytes=24 * MIB),
    )(pltpu.with_memory_space_constraint(arrived, pltpu.VMEM), hidden, w_gate, w_proj, gain)


def shards(train_table, token_ids, hidden, w_gate, w_proj, gain):
    columns, vocab = train_table.shape[1:]
    parts = ROWS * COLS
    halves, tiles = columns // 8, vocab // LANES
    table = train_table.reshape(halves, 2, SUBLANES, tiles, LANES)
    table = jnp.transpose(table, (0, 3, 1, 2, 4)).reshape(halves, parts, 2 * tiles // parts, SUBLANES, LANES)
    blocks = head(token_ids, table)
    arrived = lax.all_to_all(blocks, ("row", "col"), split_axis=0, concat_axis=0, tiled=True)
    served, update = tail(arrived, hidden, w_gate, w_proj, gain)
    served = served.reshape(ROWS, COLS, halves, tiles // parts, 2, SUBLANES, LANES)
    served = jnp.transpose(served, (0, 1, 2, 4, 5, 3, 6)).reshape(ROWS, COLS * columns, vocab // parts)
    return (served, update)


def solution(mesh):
    in_specs = (
        P("row", "col", None),
        P(),
        P("row", "col", None),
        P("row", None, None),
        P("row", None, None),
        P("row", None),
    )
    out_specs = (P(None, None, ("row", "col")), P("row", "col", None))
    return jax.shard_map(shards, mesh=mesh, in_specs=in_specs, out_specs=out_specs, check_vma=False)
```

```python
import jax
import jax.numpy as jnp
from jax import lax
from jax.experimental import pallas as pl
from jax.experimental.pallas import tpu as pltpu
from jax.sharding import PartitionSpec as P

LANES = 128
SUBLANES = 4
MIB = 1 << 20
ROWS, COLS = 8, 16
SPOT0 = 102
STEP_X, STEP_Y, STEP_Z, STEP_C = 8, -2, -32, 1


def spot(device):
    x, y = device >> 5, ((device >> 3) & 1) * 2 + ((device >> 4) & 1)
    z, core = (device >> 1) & 3, device & 1
    return SPOT0 + x * STEP_X + y * STEP_Y + z * STEP_Z + core * STEP_C


def in_hbm(array):
    return pltpu.with_memory_space_constraint(array, pltpu.HBM)


def head_kernel(ids_ref, table_ref, out_ref, place_of, ids, tile_of, turn_of, sem, ids_sem):
    halves, parts, local = table_ref.shape[:3]
    tokens = ids.shape[0]
    fetch = pltpu.make_async_copy(ids_ref, ids, ids_sem)
    fetch.start()
    for device in range(0, parts, 2):
        for h in range(halves):
            pltpu.make_async_copy(
                table_ref.at[h, pl.ds(device, 2)],
                out_ref.at[pl.ds(spot(device), 2), pl.ds(h * local, local)],
                sem,
            ).start()

    @pl.loop(0, parts, unroll=8)
    def _(device):
        place_of[device] = spot(device) * (halves * local + 1)

    fetch.wait()

    @pl.loop(0, tokens, unroll=8)
    def _(t):
        at = ids[t]
        inner = lax.bitwise_and(lax.shift_right_logical(at, 6), local - 2)
        tile_of[t] = place_of[lax.shift_right_logical(at, 11)] + inner
        turn_of[t] = lax.bitwise_and(t - at, LANES - 1)

    flat = out_ref.reshape(parts * (halves * local + 1), SUBLANES, LANES)
    whole = out_ref.at[:, pl.ds(0, halves * local)]
    pltpu.make_async_copy(whole, whole, sem).wait()

    row = lax.axis_index("row")
    lane = lax.broadcasted_iota(jnp.int32, (SUBLANES, LANES), 1)
    here = tokens // COLS
    peers = LANES // here

    @pl.loop(0, tokens // LANES)
    def _(block):
        accs = [jnp.zeros((SUBLANES, LANES), jnp.float32)] * (2 * halves)
        for i in range(LANES):
            tile, turn = tile_of[block * LANES + i], turn_of[block * LANES + i]
            for k in range(2 * halves):
                turned = pltpu.roll(flat[tile + k // 2 * local + k % 2].astype(jnp.float32), turn, 1)
                accs[k] = jnp.where(lane == i, turned, accs[k])
        accs = [pltpu.roll(acc, k * here, 1) if k else acc for k, acc in enumerate(accs)]
        for s in range(peers):
            packed = accs[-1]
            for k in range(2 * halves - 1):
                packed = jnp.where(lane // here == (s + k) % peers, accs[k], packed)
            flat[place_of[row * COLS + block * peers + s] + halves * local] = packed.astype(jnp.bfloat16)


def head(token_ids, table):
    halves, parts, local = table.shape[:3]
    tokens = token_ids.shape[0]
    return pl.pallas_call(
        head_kernel,
        out_shape=pltpu.VMEM((parts, halves * local + 1, SUBLANES, LANES), jnp.bfloat16),
        in_specs=[pl.BlockSpec(memory_space=pl.ANY)] * 2,
        out_specs=pl.BlockSpec(memory_space=pltpu.VMEM),
        scratch_shapes=[pltpu.SMEM((parts,), jnp.int32)] + [pltpu.SMEM((tokens,), jnp.int32)] * 3 + [pltpu.SemaphoreType.DMA] * 2,
        cost_estimate=pl.CostEstimate(flops=20 * MIB, bytes_accessed=16 * MIB, transcendentals=0),
        compiler_params=pltpu.CompilerParams(vmem_limit_bytes=16 * MIB),
    )(in_hbm(token_ids), in_hbm(table))


def tail_kernel(arrived_ref, hidden_ref, gate_ref, proj_ref, gain_ref, served_ref, update_ref, emb_ref, branch_ref, sems, update_sem):
    tiles = arrived_ref.shape[1]
    halfway = ROWS // 2

    @pl.loop(0, ROWS)
    def _(row):
        @pl.loop(0, COLS, unroll=8)
        def _(col):
            pltpu.make_async_copy(
                arrived_ref.at[spot(row * COLS + col), pl.ds(0, tiles - 1)], served_ref.at[row, col], sems.at[row // halfway]
            ).start()

    gate_pre = jnp.dot(hidden_ref[0], gate_ref[0], preferred_element_type=jnp.float32)
    gated = jax.nn.gelu(gate_pre, approximate=True)
    here = gated.shape[0]
    me, share = lax.axis_index("col"), LANES // here
    row = lax.axis_index("row")
    turn = lax.rem(share - lax.rem(me, share), share) * here
    for col in range(COLS):
        tile = arrived_ref[spot(row * COLS + col), tiles - 1].astype(jnp.float32)
        low = pltpu.roll(tile, turn, 1)
        for k in range(share):
            start = (col * share + k) * SUBLANES
            emb_ref[start:start + SUBLANES] = pltpu.roll(low, (LANES - k * here) % LANES, 1) if k else low
    emb = jnp.transpose(emb_ref[...])[:here]
    mixed = (gated * emb).astype(jnp.bfloat16)
    projected = jnp.dot(mixed, proj_ref[0], preferred_element_type=jnp.float32)
    inverse_rms = lax.rsqrt(jnp.mean(projected * projected, axis=-1, keepdims=True) + 1e-06)
    branch_ref[0] = (projected * inverse_rms * gain_ref[...].astype(jnp.float32)).astype(jnp.bfloat16)
    first, second = served_ref.at[pl.ds(0, halfway)], served_ref.at[pl.ds(halfway, halfway)]
    pltpu.make_async_copy(first, first, sems.at[0]).wait()
    send = pltpu.make_async_copy(branch_ref, update_ref, update_sem)
    send.start()
    pltpu.make_async_copy(second, second, sems.at[1]).wait()
    send.wait()


def tail(arrived, hidden, w_gate, w_proj, gain):
    tiles = arrived.shape[1] - 1
    return pl.pallas_call(
        tail_kernel,
        out_shape=[
            pltpu.HBM((ROWS, COLS, tiles, SUBLANES, LANES), jnp.bfloat16),
            pltpu.HBM(hidden.shape, jnp.bfloat16),
        ],
        in_specs=[pl.BlockSpec(memory_space=pltpu.VMEM)] * 5,
        out_specs=[pl.BlockSpec(memory_space=pl.ANY)] * 2,
        scratch_shapes=[
            pltpu.VMEM((w_gate.shape[2], LANES), jnp.float32),
            pltpu.VMEM(hidden.shape, jnp.bfloat16),
            pltpu.SemaphoreType.DMA((2,)),
            pltpu.SemaphoreType.DMA,
        ],
        cost_estimate=pl.CostEstimate(flops=100 * MIB, bytes_accessed=18 * MIB, transcendentals=0),
        compiler_params=pltpu.CompilerParams(vmem_limit_bytes=24 * MIB),
    )(pltpu.with_memory_space_constraint(arrived, pltpu.VMEM), hidden, w_gate, w_proj, gain)


def shards(train_table, token_ids, hidden, w_gate, w_proj, gain):
    columns, vocab = train_table.shape[1:]
    parts = ROWS * COLS
    halves, tiles = columns // 8, vocab // LANES
    table = train_table.reshape(halves, 2, SUBLANES, tiles, LANES)
    table = jnp.transpose(table, (0, 3, 1, 2, 4)).reshape(halves, parts, 2 * tiles // parts, SUBLANES, LANES)
    blocks = head(token_ids, table)
    order = sorted(range(parts), key=spot)
    arrived = lax.all_to_all(
        blocks, ("row", "col"), split_axis=0, concat_axis=0, axis_index_groups=[order], tiled=True
    )
    served, update = tail(arrived, hidden, w_gate, w_proj, gain)
    served = served.reshape(ROWS, COLS, halves, tiles // parts, 2, SUBLANES, LANES)
    served = jnp.transpose(served, (0, 1, 2, 4, 5, 3, 6)).reshape(ROWS, COLS * columns, vocab // parts)
    return (served, update)


def solution(mesh):
    in_specs = (
        P("row", "col", None),
        P(),
        P("row", "col", None),
        P("row", None, None),
        P("row", None, None),
        P("row", None),
    )
    out_specs = (P(None, None, ("row", "col")), P("row", "col", None))
    return jax.shard_map(shards, mesh=mesh, in_specs=in_specs, out_specs=out_specs, check_vma=False)
```

```python
import jax
import jax.numpy as jnp
from jax import lax
from jax.experimental import pallas as pl
from jax.experimental.pallas import tpu as pltpu
from jax.sharding import PartitionSpec as P

LANES = 128
SUBLANES = 4
MIB = 1 << 20
ROWS, COLS = 8, 16
SPOT0 = 102
STEP_X, STEP_Y, STEP_Z, STEP_C = 8, -2, -32, 1


def spot(device):
    x, y = device >> 5, ((device >> 3) & 1) * 2 + ((device >> 4) & 1)
    z, core = (device >> 1) & 3, device & 1
    return SPOT0 + x * STEP_X + y * STEP_Y + z * STEP_Z + core * STEP_C


def in_hbm(array):
    return pltpu.with_memory_space_constraint(array, pltpu.HBM)


def head_kernel(ids_ref, table_ref, out_ref, place_of, ids, tile_of, turn_of, sem, ids_sem):
    halves, parts, local = table_ref.shape[:3]
    tokens = ids.shape[0]
    fetch = pltpu.make_async_copy(ids_ref, ids, ids_sem)
    fetch.start()
    for device in range(parts):
        for h in range(halves):
            pltpu.make_async_copy(
                table_ref.at[h, device],
                out_ref.at[spot(device), pl.ds(h * local, local)],
                sem,
            ).start()

    @pl.loop(0, parts, unroll=8)
    def _(device):
        place_of[device] = spot(device) * (halves * local + 1)

    fetch.wait()

    @pl.loop(0, tokens, unroll=8)
    def _(t):
        at = ids[t]
        inner = lax.bitwise_and(lax.shift_right_logical(at, 6), local - 2)
        tile_of[t] = place_of[lax.shift_right_logical(at, 11)] + inner
        turn_of[t] = lax.bitwise_and(t - at, LANES - 1)

    flat = out_ref.reshape(parts * (halves * local + 1), SUBLANES, LANES)
    whole = out_ref.at[:, pl.ds(0, halves * local)]
    pltpu.make_async_copy(whole, whole, sem).wait()

    row = lax.axis_index("row")
    lane = lax.broadcasted_iota(jnp.int32, (SUBLANES, LANES), 1)
    wide = lax.broadcasted_iota(jnp.int32, (2 * SUBLANES, LANES), 1)
    here = tokens // COLS
    peers = LANES // here

    @pl.loop(0, tokens // LANES)
    def _(block):
        accs = [jnp.zeros((2 * SUBLANES, LANES), jnp.float32)] * halves
        for i in range(LANES):
            tile, turn = tile_of[block * LANES + i], turn_of[block * LANES + i]
            for h in range(halves):
                pair = flat[pl.ds(tile + h * local, 2)].astype(jnp.float32).reshape(2 * SUBLANES, LANES)
                accs[h] = jnp.where(wide == i, pltpu.roll(pair, turn, 1), accs[h])
        accs = [acc[q * SUBLANES:(q + 1) * SUBLANES] for acc in accs for q in range(2)]
        accs = [pltpu.roll(acc, k * here, 1) if k else acc for k, acc in enumerate(accs)]
        for s in range(peers):
            packed = accs[-1]
            for k in range(2 * halves - 1):
                packed = jnp.where(lane // here == (s + k) % peers, accs[k], packed)
            flat[place_of[row * COLS + block * peers + s] + halves * local] = packed.astype(jnp.bfloat16)


def head(token_ids, table):
    halves, parts, local = table.shape[:3]
    tokens = token_ids.shape[0]
    return pl.pallas_call(
        head_kernel,
        out_shape=pltpu.VMEM((parts, halves * local + 1, SUBLANES, LANES), jnp.bfloat16),
        in_specs=[pl.BlockSpec(memory_space=pl.ANY)] * 2,
        out_specs=pl.BlockSpec(memory_space=pltpu.VMEM),
        scratch_shapes=[pltpu.SMEM((parts,), jnp.int32)] + [pltpu.SMEM((tokens,), jnp.int32)] * 3 + [pltpu.SemaphoreType.DMA] * 2,
        cost_estimate=pl.CostEstimate(flops=20 * MIB, bytes_accessed=16 * MIB, transcendentals=0),
        compiler_params=pltpu.CompilerParams(vmem_limit_bytes=16 * MIB),
    )(in_hbm(token_ids), in_hbm(table))


def tail_kernel(arrived_ref, hidden_ref, gate_ref, proj_ref, gain_ref, served_ref, update_ref, emb_ref, branch_ref, sems, update_sem):
    tiles = arrived_ref.shape[1]
    halfway = ROWS // 2

    @pl.loop(0, ROWS)
    def _(row):
        @pl.loop(0, COLS, unroll=8)
        def _(col):
            pltpu.make_async_copy(
                arrived_ref.at[spot(row * COLS + col), pl.ds(0, tiles - 1)], served_ref.at[row, col], sems.at[row // halfway]
            ).start()

    gate_pre = jnp.dot(hidden_ref[0], gate_ref[0], preferred_element_type=jnp.float32)
    gated = jax.nn.gelu(gate_pre, approximate=True)
    here = gated.shape[0]
    me, share = lax.axis_index("col"), LANES // here
    row = lax.axis_index("row")
    turn = lax.rem(share - lax.rem(me, share), share) * here
    for col in range(COLS):
        tile = arrived_ref[spot(row * COLS + col), tiles - 1].astype(jnp.float32)
        low = pltpu.roll(tile, turn, 1)
        for k in range(share):
            start = (col * share + k) * SUBLANES
            emb_ref[start:start + SUBLANES] = pltpu.roll(low, (LANES - k * here) % LANES, 1) if k else low
    emb = jnp.transpose(emb_ref[...])[:here]
    mixed = (gated * emb).astype(jnp.bfloat16)
    projected = jnp.dot(mixed, proj_ref[0], preferred_element_type=jnp.float32)
    inverse_rms = lax.rsqrt(jnp.mean(projected * projected, axis=-1, keepdims=True) + 1e-06)
    branch_ref[0] = (projected * inverse_rms * gain_ref[...].astype(jnp.float32)).astype(jnp.bfloat16)
    first, second = served_ref.at[pl.ds(0, halfway)], served_ref.at[pl.ds(halfway, halfway)]
    pltpu.make_async_copy(first, first, sems.at[0]).wait()
    send = pltpu.make_async_copy(branch_ref, update_ref, update_sem)
    send.start()
    pltpu.make_async_copy(second, second, sems.at[1]).wait()
    send.wait()


def tail(arrived, hidden, w_gate, w_proj, gain):
    tiles = arrived.shape[1] - 1
    return pl.pallas_call(
        tail_kernel,
        out_shape=[
            pltpu.HBM((ROWS, COLS, tiles, SUBLANES, LANES), jnp.bfloat16),
            pltpu.HBM(hidden.shape, jnp.bfloat16),
        ],
        in_specs=[pl.BlockSpec(memory_space=pltpu.VMEM)] * 5,
        out_specs=[pl.BlockSpec(memory_space=pl.ANY)] * 2,
        scratch_shapes=[
            pltpu.VMEM((w_gate.shape[2], LANES), jnp.float32),
            pltpu.VMEM(hidden.shape, jnp.bfloat16),
            pltpu.SemaphoreType.DMA((2,)),
            pltpu.SemaphoreType.DMA,
        ],
        cost_estimate=pl.CostEstimate(flops=100 * MIB, bytes_accessed=18 * MIB, transcendentals=0),
        compiler_params=pltpu.CompilerParams(vmem_limit_bytes=24 * MIB),
    )(pltpu.with_memory_space_constraint(arrived, pltpu.VMEM), hidden, w_gate, w_proj, gain)


def shards(train_table, token_ids, hidden, w_gate, w_proj, gain):
    columns, vocab = train_table.shape[1:]
    parts = ROWS * COLS
    halves, tiles = columns // 8, vocab // LANES
    table = train_table.reshape(halves, 2, SUBLANES, tiles, LANES)
    table = jnp.transpose(table, (0, 3, 1, 2, 4)).reshape(halves, parts, 2 * tiles // parts, SUBLANES, LANES)
    blocks = head(token_ids, table)
    order = sorted(range(parts), key=spot)
    arrived = lax.all_to_all(
        blocks, ("row", "col"), split_axis=0, concat_axis=0, axis_index_groups=[order], tiled=True
    )
    served, update = tail(arrived, hidden, w_gate, w_proj, gain)
    served = served.reshape(ROWS, COLS, halves, tiles // parts, 2, SUBLANES, LANES)
    served = jnp.transpose(served, (0, 1, 2, 4, 5, 3, 6)).reshape(ROWS, COLS * columns, vocab // parts)
    return (served, update)


def solution(mesh):
    in_specs = (
        P("row", "col", None),
        P(),
        P("row", "col", None),
        P("row", None, None),
        P("row", None, None),
        P("row", None),
    )
    out_specs = (P(None, None, ("row", "col")), P("row", "col", None))
    return jax.shard_map(shards, mesh=mesh, in_specs=in_specs, out_specs=out_specs, check_vma=False)
```

```python
import jax
import jax.numpy as jnp
from jax import lax
from jax.experimental import pallas as pl
from jax.experimental.pallas import tpu as pltpu
from jax.sharding import PartitionSpec as P

LANES = 128
SUBLANES = 4
MIB = 1 << 20
ROWS, COLS = 8, 16
SPOT0 = 102
STEP_X, STEP_Y, STEP_Z, STEP_C = 8, -2, -32, 1


def spot(device):
    x, y = device >> 5, ((device >> 3) & 1) * 2 + ((device >> 4) & 1)
    z, core = (device >> 1) & 3, device & 1
    return SPOT0 + x * STEP_X + y * STEP_Y + z * STEP_Z + core * STEP_C


def in_hbm(array):
    return pltpu.with_memory_space_constraint(array, pltpu.HBM)


def head_kernel(ids_ref, table_ref, out_ref, place_of, ids, tile_of, turn_of, sem, ids_sem):
    halves, parts, local = table_ref.shape[:3]
    tokens = ids.shape[0]
    fetch = pltpu.make_async_copy(ids_ref, ids, ids_sem)
    fetch.start()
    for device in range(parts):
        for h in range(halves):
            pltpu.make_async_copy(
                table_ref.at[h, device],
                out_ref.at[spot(device), pl.ds(h * local, local)],
                sem,
            ).start()

    @pl.loop(0, parts, unroll=8)
    def _(device):
        place_of[device] = spot(device) * (halves * local + 1)

    fetch.wait()

    @pl.loop(0, tokens, unroll=8)
    def _(t):
        at = ids[t]
        inner = lax.bitwise_and(lax.shift_right_logical(at, 6), local - 2)
        tile_of[t] = place_of[lax.shift_right_logical(at, 11)] + inner
        turn_of[t] = lax.bitwise_and(t - at, LANES - 1)

    flat = out_ref.reshape(parts * (halves * local + 1), SUBLANES, LANES)
    whole = out_ref.at[:, pl.ds(0, halves * local)]
    pltpu.make_async_copy(whole, whole, sem).wait()

    row = lax.axis_index("row")
    lane = lax.broadcasted_iota(jnp.int32, (SUBLANES, LANES), 1)
    wide = lax.broadcasted_iota(jnp.int32, (2 * SUBLANES, LANES), 1)
    here = tokens // COLS
    peers = LANES // here

    for block in range(tokens // LANES):
        accs = [jnp.zeros((2 * SUBLANES, LANES), jnp.float32)] * halves
        for i in range(LANES):
            tile, turn = tile_of[block * LANES + i], turn_of[block * LANES + i]
            for h in range(halves):
                pair = flat[pl.ds(tile + h * local, 2)].astype(jnp.float32).reshape(2 * SUBLANES, LANES)
                accs[h] = jnp.where(wide == i, pltpu.roll(pair, turn, 1), accs[h])
        accs = [acc[q * SUBLANES:(q + 1) * SUBLANES] for acc in accs for q in range(2)]
        accs = [pltpu.roll(acc, k * here, 1) if k else acc for k, acc in enumerate(accs)]
        for s in range(peers):
            packed = accs[-1]
            for k in range(2 * halves - 1):
                packed = jnp.where(lane // here == (s + k) % peers, accs[k], packed)
            flat[place_of[row * COLS + block * peers + s] + halves * local] = packed.astype(jnp.bfloat16)


def head(token_ids, table):
    halves, parts, local = table.shape[:3]
    tokens = token_ids.shape[0]
    return pl.pallas_call(
        head_kernel,
        out_shape=pltpu.VMEM((parts, halves * local + 1, SUBLANES, LANES), jnp.bfloat16),
        in_specs=[pl.BlockSpec(memory_space=pl.ANY)] * 2,
        out_specs=pl.BlockSpec(memory_space=pltpu.VMEM),
        scratch_shapes=[pltpu.SMEM((parts,), jnp.int32)] + [pltpu.SMEM((tokens,), jnp.int32)] * 3 + [pltpu.SemaphoreType.DMA] * 2,
        cost_estimate=pl.CostEstimate(flops=20 * MIB, bytes_accessed=16 * MIB, transcendentals=0),
        compiler_params=pltpu.CompilerParams(vmem_limit_bytes=16 * MIB),
    )(in_hbm(token_ids), in_hbm(table))


def tail_kernel(arrived_ref, hidden_ref, gate_ref, proj_ref, gain_ref, served_ref, update_ref, emb_ref, branch_ref, sems, update_sem):
    tiles = arrived_ref.shape[1]
    halfway = ROWS // 2

    @pl.loop(0, ROWS)
    def _(row):
        @pl.loop(0, COLS, unroll=8)
        def _(col):
            pltpu.make_async_copy(
                arrived_ref.at[spot(row * COLS + col), pl.ds(0, tiles - 1)], served_ref.at[row, col], sems.at[row // halfway]
            ).start()

    gate_pre = jnp.dot(hidden_ref[0], gate_ref[0], preferred_element_type=jnp.float32)
    gated = jax.nn.gelu(gate_pre, approximate=True)
    here = gated.shape[0]
    me, share = lax.axis_index("col"), LANES // here
    row = lax.axis_index("row")
    turn = lax.rem(share - lax.rem(me, share), share) * here
    for col in range(COLS):
        tile = arrived_ref[spot(row * COLS + col), tiles - 1].astype(jnp.float32)
        low = pltpu.roll(tile, turn, 1)
        for k in range(share):
            start = (col * share + k) * SUBLANES
            emb_ref[start:start + SUBLANES] = pltpu.roll(low, (LANES - k * here) % LANES, 1) if k else low
    emb = jnp.transpose(emb_ref[...])[:here]
    mixed = (gated * emb).astype(jnp.bfloat16)
    projected = jnp.dot(mixed, proj_ref[0], preferred_element_type=jnp.float32)
    inverse_rms = lax.rsqrt(jnp.mean(projected * projected, axis=-1, keepdims=True) + 1e-06)
    branch_ref[0] = (projected * inverse_rms * gain_ref[...].astype(jnp.float32)).astype(jnp.bfloat16)
    first, second = served_ref.at[pl.ds(0, halfway)], served_ref.at[pl.ds(halfway, halfway)]
    pltpu.make_async_copy(first, first, sems.at[0]).wait()
    send = pltpu.make_async_copy(branch_ref, update_ref, update_sem)
    send.start()
    pltpu.make_async_copy(second, second, sems.at[1]).wait()
    send.wait()


def tail(arrived, hidden, w_gate, w_proj, gain):
    tiles = arrived.shape[1] - 1
    return pl.pallas_call(
        tail_kernel,
        out_shape=[
            pltpu.HBM((ROWS, COLS, tiles, SUBLANES, LANES), jnp.bfloat16),
            pltpu.HBM(hidden.shape, jnp.bfloat16),
        ],
        in_specs=[pl.BlockSpec(memory_space=pltpu.VMEM)] * 5,
        out_specs=[pl.BlockSpec(memory_space=pl.ANY)] * 2,
        scratch_shapes=[
            pltpu.VMEM((w_gate.shape[2], LANES), jnp.float32),
            pltpu.VMEM(hidden.shape, jnp.bfloat16),
            pltpu.SemaphoreType.DMA((2,)),
            pltpu.SemaphoreType.DMA,
        ],
        cost_estimate=pl.CostEstimate(flops=100 * MIB, bytes_accessed=18 * MIB, transcendentals=0),
        compiler_params=pltpu.CompilerParams(vmem_limit_bytes=24 * MIB),
    )(pltpu.with_memory_space_constraint(arrived, pltpu.VMEM), hidden, w_gate, w_proj, gain)


def shards(train_table, token_ids, hidden, w_gate, w_proj, gain):
    columns, vocab = train_table.shape[1:]
    parts = ROWS * COLS
    halves, tiles = columns // 8, vocab // LANES
    table = train_table.reshape(halves, 2, SUBLANES, tiles, LANES)
    table = jnp.transpose(table, (0, 3, 1, 2, 4)).reshape(halves, parts, 2 * tiles // parts, SUBLANES, LANES)
    blocks = head(token_ids, table)
    order = sorted(range(parts), key=spot)
    arrived = lax.all_to_all(
        blocks, ("row", "col"), split_axis=0, concat_axis=0, axis_index_groups=[order], tiled=True
    )
    served, update = tail(arrived, hidden, w_gate, w_proj, gain)
    served = served.reshape(ROWS, COLS, halves, tiles // parts, 2, SUBLANES, LANES)
    served = jnp.transpose(served, (0, 1, 2, 4, 5, 3, 6)).reshape(ROWS, COLS * columns, vocab // parts)
    return (served, update)


def solution(mesh):
    in_specs = (
        P("row", "col", None),
        P(),
        P("row", "col", None),
        P("row", None, None),
        P("row", None, None),
        P("row", None),
    )
    out_specs = (P(None, None, ("row", "col")), P("row", "col", None))
    return jax.shard_map(shards, mesh=mesh, in_specs=in_specs, out_specs=out_specs, check_vma=False)
```

```python
import jax
import jax.numpy as jnp
from jax import lax
from jax.experimental import pallas as pl
from jax.experimental.pallas import tpu as pltpu
from jax.sharding import PartitionSpec as P

LANES = 128
SUBLANES = 4
MIB = 1 << 20
ROWS, COLS = 8, 16
SPOT0 = 120
STEP_X, STEP_Y, STEP_Z, STEP_C = 2, -8, -32, 1


def spot(device):
    x, y = device >> 5, ((device >> 3) & 1) * 2 + ((device >> 4) & 1)
    z, core = (device >> 1) & 3, device & 1
    return SPOT0 + x * STEP_X + y * STEP_Y + z * STEP_Z + core * STEP_C


def in_hbm(array):
    return pltpu.with_memory_space_constraint(array, pltpu.HBM)


def head_kernel(ids_ref, table_ref, out_ref, place_of, ids, tile_of, turn_of, sem, ids_sem):
    halves, parts, local = table_ref.shape[:3]
    tokens = ids.shape[0]
    fetch = pltpu.make_async_copy(ids_ref, ids, ids_sem)
    fetch.start()
    for device in range(parts):
        for h in range(halves):
            pltpu.make_async_copy(
                table_ref.at[h, device],
                out_ref.at[spot(device), pl.ds(h * local, local)],
                sem,
            ).start()

    @pl.loop(0, parts, unroll=8)
    def _(device):
        place_of[device] = spot(device) * (halves * local + 1)

    fetch.wait()

    @pl.loop(0, tokens, unroll=8)
    def _(t):
        at = ids[t]
        inner = lax.bitwise_and(lax.shift_right_logical(at, 6), local - 2)
        tile_of[t] = place_of[lax.shift_right_logical(at, 11)] + inner
        turn_of[t] = lax.bitwise_and(t - at, LANES - 1)

    flat = out_ref.reshape(parts * (halves * local + 1), SUBLANES, LANES)
    whole = out_ref.at[:, pl.ds(0, halves * local)]
    pltpu.make_async_copy(whole, whole, sem).wait()

    row = lax.axis_index("row")
    lane = lax.broadcasted_iota(jnp.int32, (SUBLANES, LANES), 1)
    wide = lax.broadcasted_iota(jnp.int32, (2 * SUBLANES, LANES), 1)
    here = tokens // COLS
    peers = LANES // here

    for block in range(tokens // LANES):
        accs = [jnp.zeros((2 * SUBLANES, LANES), jnp.float32)] * halves
        for i in range(LANES):
            tile, turn = tile_of[block * LANES + i], turn_of[block * LANES + i]
            for h in range(halves):
                pair = flat[pl.ds(tile + h * local, 2)].astype(jnp.float32).reshape(2 * SUBLANES, LANES)
                accs[h] = jnp.where(wide == i, pltpu.roll(pair, turn, 1), accs[h])
        accs = [acc[q * SUBLANES:(q + 1) * SUBLANES] for acc in accs for q in range(2)]
        accs = [pltpu.roll(acc, k * here, 1) if k else acc for k, acc in enumerate(accs)]
        for s in range(peers):
            packed = accs[-1]
            for k in range(2 * halves - 1):
                packed = jnp.where(lane // here == (s + k) % peers, accs[k], packed)
            flat[place_of[row * COLS + block * peers + s] + halves * local] = packed.astype(jnp.bfloat16)


def head(token_ids, table):
    halves, parts, local = table.shape[:3]
    tokens = token_ids.shape[0]
    return pl.pallas_call(
        head_kernel,
        out_shape=pltpu.VMEM((parts, halves * local + 1, SUBLANES, LANES), jnp.bfloat16),
        in_specs=[pl.BlockSpec(memory_space=pl.ANY)] * 2,
        out_specs=pl.BlockSpec(memory_space=pltpu.VMEM),
        scratch_shapes=[pltpu.SMEM((parts,), jnp.int32)] + [pltpu.SMEM((tokens,), jnp.int32)] * 3 + [pltpu.SemaphoreType.DMA] * 2,
        cost_estimate=pl.CostEstimate(flops=20 * MIB, bytes_accessed=16 * MIB, transcendentals=0),
        compiler_params=pltpu.CompilerParams(vmem_limit_bytes=16 * MIB),
    )(in_hbm(token_ids), in_hbm(table))


def tail_kernel(arrived_ref, hidden_ref, gate_ref, proj_ref, gain_ref, served_ref, update_ref, emb_ref, branch_ref, sems, update_sem):
    tiles = arrived_ref.shape[1]
    halfway = ROWS // 2

    @pl.loop(0, ROWS)
    def _(row):
        @pl.loop(0, COLS, unroll=8)
        def _(col):
            pltpu.make_async_copy(
                arrived_ref.at[spot(row * COLS + col), pl.ds(0, tiles - 1)], served_ref.at[row, col], sems.at[row // halfway]
            ).start()

    gate_pre = jnp.dot(hidden_ref[0], gate_ref[0], preferred_element_type=jnp.float32)
    gated = jax.nn.gelu(gate_pre, approximate=True)
    here = gated.shape[0]
    me, share = lax.axis_index("col"), LANES // here
    row = lax.axis_index("row")
    turn = lax.rem(share - lax.rem(me, share), share) * here
    for col in range(COLS):
        tile = arrived_ref[spot(row * COLS + col), tiles - 1].astype(jnp.float32)
        low = pltpu.roll(tile, turn, 1)
        for k in range(share):
            start = (col * share + k) * SUBLANES
            emb_ref[start:start + SUBLANES] = pltpu.roll(low, (LANES - k * here) % LANES, 1) if k else low
    emb = jnp.transpose(emb_ref[...])[:here]
    mixed = (gated * emb).astype(jnp.bfloat16)
    projected = jnp.dot(mixed, proj_ref[0], preferred_element_type=jnp.float32)
    inverse_rms = lax.rsqrt(jnp.mean(projected * projected, axis=-1, keepdims=True) + 1e-06)
    branch_ref[0] = (projected * inverse_rms * gain_ref[...].astype(jnp.float32)).astype(jnp.bfloat16)
    first, second = served_ref.at[pl.ds(0, halfway)], served_ref.at[pl.ds(halfway, halfway)]
    pltpu.make_async_copy(first, first, sems.at[0]).wait()
    send = pltpu.make_async_copy(branch_ref, update_ref, update_sem)
    send.start()
    pltpu.make_async_copy(second, second, sems.at[1]).wait()
    send.wait()


def tail(arrived, hidden, w_gate, w_proj, gain):
    tiles = arrived.shape[1] - 1
    return pl.pallas_call(
        tail_kernel,
        out_shape=[
            pltpu.HBM((ROWS, COLS, tiles, SUBLANES, LANES), jnp.bfloat16),
            pltpu.HBM(hidden.shape, jnp.bfloat16),
        ],
        in_specs=[pl.BlockSpec(memory_space=pltpu.VMEM)] * 5,
        out_specs=[pl.BlockSpec(memory_space=pl.ANY)] * 2,
        scratch_shapes=[
            pltpu.VMEM((w_gate.shape[2], LANES), jnp.float32),
            pltpu.VMEM(hidden.shape, jnp.bfloat16),
            pltpu.SemaphoreType.DMA((2,)),
            pltpu.SemaphoreType.DMA,
        ],
        cost_estimate=pl.CostEstimate(flops=100 * MIB, bytes_accessed=18 * MIB, transcendentals=0),
        compiler_params=pltpu.CompilerParams(vmem_limit_bytes=24 * MIB),
    )(pltpu.with_memory_space_constraint(arrived, pltpu.VMEM), hidden, w_gate, w_proj, gain)


def shards(train_table, token_ids, hidden, w_gate, w_proj, gain):
    columns, vocab = train_table.shape[1:]
    parts = ROWS * COLS
    halves, tiles = columns // 8, vocab // LANES
    table = train_table.reshape(halves, 2, SUBLANES, tiles, LANES)
    table = jnp.transpose(table, (0, 3, 1, 2, 4)).reshape(halves, parts, 2 * tiles // parts, SUBLANES, LANES)
    blocks = head(token_ids, table)
    order = sorted(range(parts), key=spot)
    arrived = lax.all_to_all(
        blocks, ("row", "col"), split_axis=0, concat_axis=0, axis_index_groups=[order], tiled=True
    )
    served, update = tail(arrived, hidden, w_gate, w_proj, gain)
    served = served.reshape(ROWS, COLS, halves, tiles // parts, 2, SUBLANES, LANES)
    served = jnp.transpose(served, (0, 1, 2, 4, 5, 3, 6)).reshape(ROWS, COLS * columns, vocab // parts)
    return (served, update)


def solution(mesh):
    in_specs = (
        P("row", "col", None),
        P(),
        P("row", "col", None),
        P("row", None, None),
        P("row", None, None),
        P("row", None),
    )
    out_specs = (P(None, None, ("row", "col")), P("row", "col", None))
    return jax.shard_map(shards, mesh=mesh, in_specs=in_specs, out_specs=out_specs, check_vma=False)
```
